32 devices in a mesh: chrom: 2 (over y), var: 16 (over z, x, core).
Axes of the slice: x: 2, y: 2, z: 4, core: 2. Of those that a mesh axis runs over, the one named last changes fastest.
Arguments:
- genotypes: bfloat16 [2048, 16384], P(None, ('chrom', 'var')), parts along dimension 1, may hold values from -6 to 6
- weights: float32 [512, 32, 3072], P(('chrom', 'var')), parts along dimension 0, may hold values from -0.109375 to 0.109375
- starts: int32 [512], P(('chrom', 'var')), parts along dimension 0, may hold values from 0 to 8191, as said below
- ends: int32 [512], P(('chrom', 'var')), parts along dimension 0, may hold values from 1 to 8192, as said below
- phenotypes: float32 [2048, 32], replicated, may hold values from -6 to 6
Outputs:
- scores: float32 [512, 1024], P(('chrom', 'var')), parts along dimension 0
- linkage: bfloat16 [16384, 1536], P(('chrom', 'var')), parts along dimension 0
The draws below stay inside these ranges and needn't reach their ends.
There are 2 independent parts, one for each index of `chrom`. The reference program is written for one: setup_inputs(seed, part) draws one part's arguments, and reference() takes and returns one part's arrays. A program takes and returns all parts, laid end to end along the dimension named above; an argument that names none is the same for every part. Nothing has to cross between parts.
Inputs may be any that keep to these rules, and one draw needn't show every extreme that they name: starts[g] lies between (g // 16) * 512 and (g // 16) * 512 + 511. ends[g] - starts[g] is between 1 and 3072, equals 3072 for gene 0, and ends[g] <= 8192.
All inputs are finite; a program needn't handle non-finite values.
Results may differ from the reference program's by a relative error of at most 0.0057.
Values may be sent and summed in bfloat16 or wider, within the bound.
A program may use at most 128 MiB of HBM per device.

```python
import jax
import jax.numpy as jnp
from jax import lax

SAMPLES = 2048
VB = 512
V = 8192
GENE_DEV = 16
GENES = 256
TISSUES = 32
PHENO = 32
WMAX = 3072
WMIN = 1024
REACH = 6


def draw_genotypes(key, part):
    noise = jax.random.normal(jax.random.fold_in(key, 11), (SAMPLES, V), jnp.float32)
    return jnp.clip(noise, -6.0, 6.0).astype(jnp.bfloat16)


def window_bounds(key):
    base = jax.random.fold_in(key, 5)
    gene_index = jnp.arange(GENES, dtype=jnp.int32)
    block_index = gene_index // GENE_DEV
    offsets = jax.random.randint(jax.random.fold_in(base, 1), (GENES,), 0, VB, jnp.int32)
    lengths = jax.random.randint(jax.random.fold_in(base, 2), (GENES,), WMIN, WMAX + 1, jnp.int32)
    lengths = jnp.where(gene_index % GENE_DEV == 0, WMAX, lengths)
    first = block_index * VB + offsets
    last = jnp.minimum(first + lengths, V)
    return (first.astype(jnp.int32), last.astype(jnp.int32))


def draw_starts(key, part):
    return window_bounds(key)[0]


def draw_ends(key, part):
    return window_bounds(key)[1]


def levels(stream_key, shape, cuts, least, high):
    gain = 1.0
    for dim, shards_of in cuts:
        draws = jax.random.uniform(jax.random.fold_in(jax.random.fold_in(stream_key, 6), dim), (shards_of,), jnp.float32, least / len(cuts), high / len(cuts))
        gain = gain * jnp.repeat(jnp.exp(draws), shape[dim] // shards_of).reshape((-1,) + (1,) * (len(shape) - 1 - dim))
    return gain


def normal_values(own_key, shape, scale, most, pieces=(), kind=jnp.bfloat16):
    drawn = jax.random.normal(own_key, shape, jnp.float32) * scale
    if len(pieces) > 0:
        drawn = levels(own_key, shape, pieces, -0.22, 0.18) * drawn
    return jnp.clip(drawn, min=-most, max=most).astype(kind)


def setup_inputs(seed: int = 0, part: int = 0) -> dict:
    arg_keys = jax.random.split(jax.random.key(seed), 6)
    part_splits = jax.random.split(jax.random.fold_in(arg_keys[5], part), 6)
    return {
        "genotypes": draw_genotypes(jax.random.fold_in(jax.random.fold_in(arg_keys[5], part), 71), part),
        "weights": normal_values(part_splits[1], (GENES, TISSUES, WMAX), WMAX ** -0.5, 0.109375, ((0, 16),), jnp.float32),
        "starts": draw_starts(jax.random.fold_in(jax.random.fold_in(arg_keys[5], part), 71), part),
        "ends": draw_ends(jax.random.fold_in(jax.random.fold_in(arg_keys[5], part), 71), part),
        "phenotypes": normal_values(arg_keys[4], (SAMPLES, PHENO), 1.0, 6.0, (), jnp.float32),
    }


EPSILON = 1e-05

def standardize(values):
    centre = lax.optimization_barrier(jnp.mean(values, axis=0))
    centred = values - centre
    spread = lax.optimization_barrier(jnp.mean(centred * centred, axis=0))
    return (centred * lax.rsqrt(spread + EPSILON)).astype(jnp.bfloat16)

def place_weights(gene_weights, gene_starts, gene_ends, anchor, window_cols):
    span = gene_weights.shape[2]
    column = jnp.arange(span, dtype=jnp.int32)
    lengths = (gene_ends - gene_starts).astype(jnp.int32)
    rounded = gene_weights.astype(jnp.bfloat16)
    masked = jnp.where(column[None, None, :] < lengths[:, None, None], rounded, jnp.zeros_like(rounded))
    padded = jnp.pad(masked, ((0, 0), (0, 0), (window_cols, window_cols - span)))
    offsets = (gene_starts - anchor).astype(jnp.int32)

    def place_one(single, offset):
        return lax.dynamic_slice_in_dim(single, (window_cols - offset).astype(jnp.int32), window_cols, 1)
    placed = jax.vmap(place_one)(padded, offsets)
    return placed.reshape(-1, window_cols)

def reference(genotypes, weights, starts, ends, phenotypes):
    window_cols = (REACH + 1) * VB
    blocks = GENES // GENE_DEV
    gene_cols = GENE_DEV * TISSUES
    padded = jnp.concatenate([genotypes, jnp.zeros((SAMPLES, REACH * VB), genotypes.dtype)], axis=1)

    def one_block(block_index):
        region = lax.dynamic_slice_in_dim(padded, (block_index * VB).astype(jnp.int32), window_cols, 1)
        first_gene = (block_index * GENE_DEV).astype(jnp.int32)
        own_weights = lax.dynamic_slice_in_dim(weights, first_gene, GENE_DEV, 0)
        own_starts = lax.dynamic_slice_in_dim(starts, first_gene, GENE_DEV, 0)
        own_ends = lax.dynamic_slice_in_dim(ends, first_gene, GENE_DEV, 0)
        placed = place_weights(own_weights, own_starts, own_ends, (block_index * VB).astype(jnp.int32), window_cols)
        return jnp.dot(region, placed.T, preferred_element_type=jnp.float32)
    expression = lax.map(one_block, jnp.arange(blocks, dtype=jnp.int32))
    expression = jnp.transpose(expression, (1, 0, 2)).reshape(SAMPLES, GENES * TISSUES)
    scaled = standardize(expression)
    pheno_scaled = standardize(phenotypes)
    scores = jnp.dot(scaled.T, pheno_scaled, preferred_element_type=jnp.float32) / jnp.sqrt(jnp.float32(SAMPLES))
    scores = scores.reshape(GENES, TISSUES * PHENO)
    bordered = jnp.pad(scaled, ((0, 0), (gene_cols, gene_cols)))

    def one_link(block_index):
        own_cols = lax.dynamic_slice_in_dim(scaled, (block_index * gene_cols).astype(jnp.int32), gene_cols, 1)
        beside_all = lax.dynamic_slice_in_dim(bordered, (block_index * gene_cols).astype(jnp.int32), 3 * gene_cols, 1)
        product = jnp.dot(own_cols.T, beside_all, preferred_element_type=jnp.float32)
        return (product / jnp.float32(SAMPLES)).astype(jnp.bfloat16)
    linkage = lax.map(one_link, jnp.arange(blocks, dtype=jnp.int32)).reshape(GENES * TISSUES, 3 * gene_cols)
    return (scores, linkage)
```

```python
import functools

import jax
import jax.numpy as jnp
from jax import lax
from jax.experimental import pallas as pl
from jax.experimental.pallas import tpu as pltpu
from jax.sharding import PartitionSpec as P

EPSILON = 1e-05
ROUND = 128
CHUNK = 128
XF, XH, ZF, ZH, PEER = 0, 1, 2, 3, 4


def dot_nt(left, right):
    return lax.dot_general(
        left, right, (((1,), (1,)), ((), ())), preferred_element_type=jnp.float32
    )


def standardize_rows(values):
    scale = 1.0 / values.shape[1]
    centred = values - jnp.sum(values, axis=1, keepdims=True) * scale
    spread = jnp.sum(centred * centred, axis=1, keepdims=True) * scale
    return (centred * lax.rsqrt(spread + EPSILON)).astype(jnp.bfloat16)


def kernel(
    n, starts_ref, ends_ref, geno_hbm, weights_hbm, pheno_ref, scores_ref, link_ref,
    wbuf, gbuf, placed, et, scaled, rx, ret_out, ret_in,
    wsem, gsem, send, recv, fsend, frecv, bsend, brecv,
):
    me = lax.axis_index("var")
    core = lax.rem(me, 2)
    col = lax.rem(lax.div(me, 2), 2)
    other = 1 - core
    genes, tissues, span = weights_hbm.shape
    samples, cols = geno_hbm.shape
    reach = span // cols
    rounds = samples // ROUND
    half = ROUND // 2
    x_peer = me + 2 - 4 * col
    sibling = me + 1 - 2 * core
    up = me + 4 < n
    down = me >= 4
    is_a = col == 0

    def weight_copy(g):
        return pltpu.make_async_copy(weights_hbm.at[g], wbuf.at[g], wsem.at[g])

    own_copy = pltpu.make_async_copy(geno_hbm, gbuf.at[core], gsem)
    own_copy.start()

    barrier = pltpu.get_barrier_semaphore()
    expected = jnp.int32(0)
    for peer in (me - 4, me + 4, me - 1, me + 1):
        exists = jnp.logical_and(peer >= 0, peer < n)
        expected = expected + exists.astype(jnp.int32)

        @pl.when(exists)
        def _():
            pl.semaphore_signal(
                barrier, inc=1, device_id={"var": peer}, device_id_type=pl.DeviceIdType.MESH
            )

    pl.semaphore_signal(
        barrier, inc=1, device_id={"var": x_peer}, device_id_type=pl.DeviceIdType.MESH
    )
    pl.semaphore_wait(barrier, expected + 1)
    own_copy.wait()

    def piece(q, j, s, part):
        if part is None:
            return gbuf.at[2 * q + j, pl.ds(s * ROUND, ROUND), :]
        return gbuf.at[2 * q + j, pl.ds(s * ROUND + part * half, half), :]

    def remote(kind, s, source, target, device):
        return pltpu.make_async_remote_copy(
            src_ref=source,
            dst_ref=target,
            send_sem=send.at[kind, s],
            recv_sem=recv.at[kind, s],
            device_id={"var": device},
            device_id_type=pl.DeviceIdType.MESH,
        )

    def out_copy(kind, s):
        if kind == XF:
            return remote(XF, s, piece(2 - 2 * col, core, s, None), piece(1, core, s, None), x_peer)
        if kind == XH:
            part = 1 - col
            return remote(
                XH, s, piece(3 - col, core, s, part), piece(2 + col, core, s, part), x_peer
            )
        if kind == ZF:
            return remote(ZF, s, piece(col, core, s, None), piece(2 + col, core, s, None), me - 4)
        if kind == ZH:
            part = 1 - col
            return remote(
                ZH, s, piece(1 - col, core, s, part), piece(3 - col, core, s, part), me - 4
            )
        q = kind - PEER + 1 - core
        return remote(kind, s, piece(q, core, s, None), piece(q, core, s, None), sibling)

    def in_copy(kind, s):
        if kind == XF:
            ref = piece(1, core, s, None)
        elif kind == XH:
            ref = piece(3 - col, core, s, col)
        elif kind == ZF:
            ref = piece(2 + col, core, s, None)
        elif kind == ZH:
            ref = piece(3 - col, core, s, 1 - col)
        else:
            ref = piece(kind - PEER + core, other, s, None)
        return remote(kind, s, ref, ref, sibling)

    in_zf = me + 4 + 4 * col < n
    in_xf = jnp.logical_or(is_a, up)
    sends = {
        XF: jnp.logical_or(col == 1, up),
        XH: up,
        ZF: jnp.logical_and(down, jnp.logical_or(is_a, up)),
        ZH: down,
    }
    recvs = {XF: in_xf, XH: up, ZF: in_zf, ZH: up}
    has = [me >= 0, in_xf, up, in_zf]
    for m in range(3):
        sends[PEER + m] = jnp.where(core == 0, has[m + 1], has[m])
        recvs[PEER + m] = jnp.where(core == 0, has[m], has[m + 1])

    def start(kind, s, *conditions):
        ok = sends[kind]
        for condition in conditions:
            ok = jnp.logical_and(ok, condition)

        @pl.when(ok)
        def _():
            out_copy(kind, s).start()

    def arrive(kind, s, *conditions):
        ok = recvs[kind]
        for condition in conditions:
            ok = jnp.logical_and(ok, condition)

        @pl.when(ok)
        def _():
            in_copy(kind, s).wait_recv()

    is_b = col == 1
    first = core == 0
    second = core == 1

    def issue_own(s, carry):
        start(ZF, s, is_a)
        start(XF, s, is_b)
        start(ZH, s, is_b)
        start(PEER, s, second)
        return carry

    lax.fori_loop(0, rounds, issue_own, 0)

    def issue_weights(g, carry):
        weight_copy(g).start()
        return carry

    lax.fori_loop(0, genes, issue_weights, 0)

    base = me * cols
    width = span + cols

    def place(g):
        weight_copy(g).wait()
        offset = starts_ref[g] - base
        stop = ends_ref[g] - base
        padded = jnp.concatenate(
            [wbuf[g], jnp.zeros((tissues, cols), jnp.float32)], axis=1
        )
        moved = pltpu.roll(padded, offset, 1)
        column = lax.broadcasted_iota(jnp.int32, (tissues, width), 1)
        inside = jnp.logical_and(column >= offset, column < stop)
        placed[pl.ds(g * tissues, tissues), :] = jnp.where(inside, moved, 0.0).astype(
            jnp.bfloat16
        )

    def relay_one(s, carry):
        arrive(ZF, s, is_a)
        start(XF, s, is_a)
        arrive(XF, s)
        start(ZH, s, is_a)
        start(ZF, s, is_b)
        start(PEER, s, first)
        start(PEER + 1, s, second)
        arrive(ZH, s, is_b)
        start(XH, s, is_b)
        start(PEER + 1, s, first, is_a)
        start(PEER + 2, s, second, is_a)
        return carry

    per_round = -(-genes // rounds)

    def first_stage(s, carry):
        relay_one(s, 0)
        for extra in range(per_round):
            g = s * per_round + extra

            @pl.when(g < genes)
            def _():
                place(g)

        return carry

    lax.fori_loop(0, rounds, first_stage, 0)

    def multiply(pair):
        rows = pl.ds(pair * 2 * ROUND, 2 * ROUND)
        for d in range(reach + 1):

            @pl.when(me + d < n)
            def _():
                product = dot_nt(placed[:, d * cols : (d + 1) * cols], gbuf[core + d, rows, :])
                if d == 0:
                    et[:, rows] = product
                else:
                    et[:, rows] += product

    def second_stage(s, carry):
        @pl.when(s < rounds)
        def _():
            arrive(ZH, s, is_a)
            start(XH, s, is_a)
            arrive(XH, s)
            start(PEER + 1, s, first, is_b)
            start(PEER + 2, s, second, is_b)
            arrive(ZF, s, is_b)
            start(PEER + 2, s, first)

        @pl.when(jnp.logical_and(s >= 2, lax.rem(s, 2) == 0))
        def _():
            for back in (2, 1):
                for m in range(3):
                    arrive(PEER + m, s - back)
            multiply(lax.div(s, 2) - 1)

        return carry

    lax.fori_loop(0, rounds + 1, second_stage, 0)

    total = placed.shape[0]
    chunks = total // CHUNK
    has_next = me < n - 1
    has_prev = me > 0

    def forward(c):
        rows = pl.ds(c * CHUNK, CHUNK)
        return pltpu.make_async_remote_copy(
            src_ref=scaled.at[rows, :],
            dst_ref=rx.at[rows, :],
            send_sem=fsend.at[c],
            recv_sem=frecv.at[c],
            device_id={"var": me + 1},
            device_id_type=pl.DeviceIdType.MESH,
        )

    def backward(c):
        rows = pl.ds(c * CHUNK, CHUNK)
        return pltpu.make_async_remote_copy(
            src_ref=ret_out.at[rows, :],
            dst_ref=ret_in.at[rows, :],
            send_sem=bsend.at[c],
            recv_sem=brecv.at[c],
            device_id={"var": me - 1},
            device_id_type=pl.DeviceIdType.MESH,
        )

    step = 32

    def standardize_chunk(c, carry):
        def some(b, inner):
            rows = pl.ds(c * CHUNK + b * step, step)
            scaled[rows, :] = standardize_rows(et[rows, :])
            return inner

        lax.fori_loop(0, CHUNK // step, some, 0)

        @pl.when(has_next)
        def _():
            forward(c).start()

        return carry

    lax.fori_loop(0, chunks, standardize_chunk, 0)

    shrink = 1.0 / samples
    pheno_scaled = standardize_rows(pheno_ref[...])
    scores_ref[...] = dot_nt(scaled[...], pheno_scaled) / jnp.sqrt(jnp.float32(samples))

    def own_block(c, carry):
        rows = pl.ds(c * CHUNK, CHUNK)
        link_ref[rows, total : 2 * total] = (dot_nt(scaled[rows, :], scaled[...]) * shrink).astype(
            jnp.bfloat16
        )
        return carry

    lax.fori_loop(0, chunks, own_block, 0)

    def before(c, carry):
        rows = pl.ds(c * CHUNK, CHUNK)

        @pl.when(has_prev)
        def _():
            forward(c).wait_recv()
            product = (dot_nt(rx[rows, :], scaled[...]) * shrink).astype(jnp.bfloat16)
            ret_out[rows, :] = product
            across = (dot_nt(scaled[...], rx[rows, :]) * shrink).astype(jnp.bfloat16)
            link_ref[:, pl.ds(pl.multiple_of(c * CHUNK, CHUNK), CHUNK)] = across
            backward(c).start()

        return carry

    lax.fori_loop(0, chunks, before, 0)

    @pl.when(jnp.logical_not(has_prev))
    def _():
        link_ref[:, :total] = jnp.zeros((total, total), jnp.bfloat16)

    @pl.when(jnp.logical_not(has_next))
    def _():
        link_ref[:, 2 * total :] = jnp.zeros((total, total), jnp.bfloat16)

    def drain(s, carry):
        for kind in range(PEER + 3):

            @pl.when(sends[kind])
            def _():
                out_copy(kind, s).wait_send()

        return carry

    lax.fori_loop(0, rounds, drain, 0)

    def after(c, carry):
        rows = pl.ds(c * CHUNK, CHUNK)

        @pl.when(has_next)
        def _():
            backward(c).wait_recv()
            link_ref[rows, 2 * total :] = ret_in[rows, :]
            forward(c).wait_send()

        @pl.when(has_prev)
        def _():
            backward(c).wait_send()

        return carry

    lax.fori_loop(0, chunks, after, 0)


def on_device(n, genotypes, weights, starts, ends, phenotypes):
    samples, cols = genotypes.shape
    genes, tissues, span = weights.shape
    total = genes * tissues
    slots = span // cols + 2
    rounds = samples // ROUND
    chunks = total // CHUNK
    vmem = pl.BlockSpec(memory_space=pltpu.VMEM)
    smem = pl.BlockSpec(memory_space=pltpu.SMEM)
    hbm = pl.BlockSpec(memory_space=pl.ANY)
    dma = pltpu.SemaphoreType.DMA
    traits = phenotypes.shape[1]
    scores, linkage = pl.pallas_call(
        functools.partial(kernel, n),
        out_shape=(
            jax.ShapeDtypeStruct((total, traits), jnp.float32),
            jax.ShapeDtypeStruct((total, 3 * total), jnp.bfloat16),
        ),
        in_specs=[smem, smem, hbm, hbm, vmem],
        out_specs=(vmem, vmem),
        scratch_shapes=[
            pltpu.VMEM((genes, tissues, span), jnp.float32),
            pltpu.VMEM((slots, samples, cols), jnp.bfloat16),
            pltpu.VMEM((total, span + cols), jnp.bfloat16),
            pltpu.VMEM((total, samples), jnp.float32),
            pltpu.VMEM((total, samples), jnp.bfloat16),
            pltpu.VMEM((total, samples), jnp.bfloat16),
            pltpu.VMEM((total, total), jnp.bfloat16),
            pltpu.VMEM((total, total), jnp.bfloat16),
            dma((genes,)),
            dma,
            dma((PEER + 3, rounds)),
            dma((PEER + 3, rounds)),
            dma((chunks,)),
            dma((chunks,)),
            dma((chunks,)),
            dma((chunks,)),
        ],
        compiler_params=pltpu.CompilerParams(
            collective_id=0, has_side_effects=True, vmem_limit_bytes=60 * 1024 * 1024
        ),
    )(starts, ends, genotypes, weights, phenotypes.T)
    return scores.reshape(genes, -1), linkage


def solution(mesh):
    placed = (
        P(None, ("chrom", "var")),
        P(("chrom", "var"), None, None),
        P(("chrom", "var")),
        P(("chrom", "var")),
        P(),
    )
    return jax.shard_map(
        functools.partial(on_device, mesh.shape["var"]),
        mesh=mesh,
        in_specs=placed,
        out_specs=(P(("chrom", "var"), None), P(("chrom", "var"), None)),
        check_vma=False,
    )
```

```python
import functools

import jax
import jax.numpy as jnp
from jax import lax
from jax.experimental import pallas as pl
from jax.experimental.pallas import tpu as pltpu
from jax.sharding import PartitionSpec as P

EPSILON = 1e-05
ROUND = 128
PRODUCT = 256
CHUNK = 64
XF, XH, ZF, ZH, PEER = 0, 1, 2, 3, 4


def dot_nt(left, right):
    return lax.dot_general(
        left, right, (((1,), (1,)), ((), ())), preferred_element_type=jnp.float32
    )


def standardize_rows(values):
    scale = 1.0 / values.shape[1]
    centred = values - jnp.sum(values, axis=1, keepdims=True) * scale
    spread = jnp.sum(centred * centred, axis=1, keepdims=True) * scale
    return (centred * lax.rsqrt(spread + EPSILON)).astype(jnp.bfloat16)


def kernel(
    n, starts_ref, ends_ref, geno_hbm, weights_hbm, pheno_ref, scores_ref, link_ref,
    wbuf, gbuf, placed, et, scaled, rx, ret_out, ret_in,
    wsem, gsem, send, recv, fsend, frecv, bsend, brecv,
):
    me = lax.axis_index("var")
    core = lax.rem(me, 2)
    col = lax.rem(lax.div(me, 2), 2)
    other = 1 - core
    genes, tissues, span = weights_hbm.shape
    samples, cols = geno_hbm.shape
    reach = span // cols
    rounds = samples // ROUND
    half = ROUND // 2
    x_peer = me + 2 - 4 * col
    sibling = me + 1 - 2 * core
    up = me + 4 < n
    down = me >= 4
    is_a = col == 0

    def weight_copy(g):
        return pltpu.make_async_copy(weights_hbm.at[g], wbuf.at[g], wsem.at[g])

    own_copy = pltpu.make_async_copy(geno_hbm, gbuf.at[core], gsem)
    own_copy.start()

    barrier = pltpu.get_barrier_semaphore()
    expected = jnp.int32(0)
    for peer in (me - 4, me + 4, me - 1, me + 1):
        exists = jnp.logical_and(peer >= 0, peer < n)
        expected = expected + exists.astype(jnp.int32)

        @pl.when(exists)
        def _():
            pl.semaphore_signal(
                barrier, inc=1, device_id={"var": peer}, device_id_type=pl.DeviceIdType.MESH
            )

    pl.semaphore_signal(
        barrier, inc=1, device_id={"var": x_peer}, device_id_type=pl.DeviceIdType.MESH
    )
    pl.semaphore_wait(barrier, expected + 1)
    own_copy.wait()

    def piece(q, j, s, part):
        if part is None:
            return gbuf.at[2 * q + j, pl.ds(s * ROUND, ROUND), :]
        return gbuf.at[2 * q + j, pl.ds(s * ROUND + part * half, half), :]

    def remote(kind, s, source, target, device):
        return pltpu.make_async_remote_copy(
            src_ref=source,
            dst_ref=target,
            send_sem=send.at[kind, s],
            recv_sem=recv.at[kind, s],
            device_id={"var": device},
            device_id_type=pl.DeviceIdType.MESH,
        )

    def out_copy(kind, s):
        if kind == XF:
            return remote(XF, s, piece(2 - 2 * col, core, s, None), piece(1, core, s, None), x_peer)
        if kind == XH:
            part = 1 - col
            return remote(
                XH, s, piece(3 - col, core, s, part), piece(2 + col, core, s, part), x_peer
            )
        if kind == ZF:
            return remote(ZF, s, piece(col, core, s, None), piece(2 + col, core, s, None), me - 4)
        if kind == ZH:
            part = 1 - col
            return remote(
                ZH, s, piece(1 - col, core, s, part), piece(3 - col, core, s, part), me - 4
            )
        q = kind - PEER + 1 - core
        return remote(kind, s, piece(q, core, s, None), piece(q, core, s, None), sibling)

    def in_copy(kind, s):
        if kind == XF:
            ref = piece(1, core, s, None)
        elif kind == XH:
            ref = piece(3 - col, core, s, col)
        elif kind == ZF:
            ref = piece(2 + col, core, s, None)
        elif kind == ZH:
            ref = piece(3 - col, core, s, 1 - col)
        else:
            ref = piece(kind - PEER + core, other, s, None)
        return remote(kind, s, ref, ref, sibling)

    in_zf = me + 4 + 4 * col < n
    in_xf = jnp.logical_or(is_a, up)
    sends = {
        XF: jnp.logical_or(col == 1, up),
        XH: up,
        ZF: jnp.logical_and(down, jnp.logical_or(is_a, up)),
        ZH: down,
    }
    recvs = {XF: in_xf, XH: up, ZF: in_zf, ZH: up}
    has = [me >= 0, in_xf, up, in_zf]
    for m in range(3):
        sends[PEER + m] = jnp.where(core == 0, has[m + 1], has[m])
        recvs[PEER + m] = jnp.where(core == 0, has[m], has[m + 1])

    def start(kind, s, *conditions):
        ok = sends[kind]
        for condition in conditions:
            ok = jnp.logical_and(ok, condition)

        @pl.when(ok)
        def _():
            out_copy(kind, s).start()

    def arrive(kind, s, *conditions):
        ok = recvs[kind]
        for condition in conditions:
            ok = jnp.logical_and(ok, condition)

        @pl.when(ok)
        def _():
            in_copy(kind, s).wait_recv()

    is_b = col == 1
    first = core == 0
    second = core == 1

    def issue_own(s, carry):
        start(ZF, s, is_a)
        start(XF, s, is_b)
        start(ZH, s, is_b)
        start(PEER, s, second)
        return carry

    lax.fori_loop(0, rounds, issue_own, 0)

    for q in range(1, gbuf.shape[0] // 2):

        @pl.when(jnp.logical_not(has[q]))
        def _():
            def clear(s, carry):
                gbuf[2 * q : 2 * q + 2, pl.ds(s * ROUND, ROUND), :] = jnp.zeros(
                    (2, ROUND, cols), gbuf.dtype
                )
                return carry

            lax.fori_loop(0, rounds, clear, 0)

    def issue_weights(g, carry):
        weight_copy(g).start()
        return carry

    lax.fori_loop(0, genes, issue_weights, 0)

    base = me * cols
    width = span + cols

    def place(g):
        weight_copy(g).wait()
        offset = starts_ref[g] - base
        stop = ends_ref[g] - base
        padded = jnp.concatenate(
            [wbuf[g], jnp.zeros((tissues, cols), jnp.float32)], axis=1
        )
        moved = pltpu.roll(padded, offset, 1)
        column = lax.broadcasted_iota(jnp.int32, (tissues, width), 1)
        inside = jnp.logical_and(column >= offset, column < stop)
        placed[pl.ds(g * tissues, tissues), :] = jnp.where(inside, moved, 0.0).astype(
            jnp.bfloat16
        )

    def relay_one(s, carry):
        arrive(ZF, s, is_a)
        start(XF, s, is_a)
        arrive(XF, s)
        start(ZH, s, is_a)
        start(ZF, s, is_b)
        start(PEER, s, first)
        start(PEER + 1, s, second)
        arrive(ZH, s, is_b)
        start(XH, s, is_b)
        start(PEER + 1, s, first, is_a)
        start(PEER + 2, s, second, is_a)
        return carry

    per_round = -(-genes // rounds)

    def first_stage(s, carry):
        relay_one(s, 0)
        for extra in range(per_round):
            g = s * per_round + extra

            @pl.when(g < genes)
            def _():
                place(g)

        return carry

    lax.fori_loop(0, rounds, first_stage, 0)

    def multiply(pair):
        rows = pl.ds(pair * PRODUCT, PRODUCT)
        acc = dot_nt(placed[:, :cols], gbuf[core, rows, :])
        for d in range(1, reach + 1):
            acc = acc + dot_nt(placed[:, d * cols : (d + 1) * cols], gbuf[core + d, rows, :])
        et[:, rows] = acc

    group = PRODUCT // ROUND

    def second_stage(s, carry):
        @pl.when(s < rounds)
        def _():
            arrive(ZH, s, is_a)
            start(XH, s, is_a)
            arrive(XH, s)
            start(PEER + 1, s, first, is_b)
            start(PEER + 2, s, second, is_b)
            arrive(ZF, s, is_b)
            start(PEER + 2, s, first)

        @pl.when(jnp.logical_and(s >= group, lax.rem(s, group) == 0))
        def _():
            for back in range(group, 0, -1):
                for m in range(3):
                    arrive(PEER + m, s - back)
            multiply(lax.div(s, group) - 1)

        return carry

    lax.fori_loop(0, rounds + 1, second_stage, 0)

    total = placed.shape[0]
    chunks = total // CHUNK
    has_next = me < n - 1
    has_prev = me > 0

    def forward(c):
        rows = pl.ds(c * CHUNK, CHUNK)
        return pltpu.make_async_remote_copy(
            src_ref=scaled.at[rows, :],
            dst_ref=rx.at[rows, :],
            send_sem=fsend.at[c],
            recv_sem=frecv.at[c],
            device_id={"var": me + 1},
            device_id_type=pl.DeviceIdType.MESH,
        )

    def backward(c):
        rows = pl.ds(c * CHUNK, CHUNK)
        return pltpu.make_async_remote_copy(
            src_ref=ret_out.at[rows, :],
            dst_ref=ret_in.at[rows, :],
            send_sem=bsend.at[c],
            recv_sem=brecv.at[c],
            device_id={"var": me - 1},
            device_id_type=pl.DeviceIdType.MESH,
        )

    step = 32

    def standardize_chunk(c, carry):
        def some(b, inner):
            rows = pl.ds(c * CHUNK + b * step, step)
            scaled[rows, :] = standardize_rows(et[rows, :])
            return inner

        lax.fori_loop(0, CHUNK // step, some, 0)

        @pl.when(has_next)
        def _():
            forward(c).start()

        return carry

    lax.fori_loop(0, chunks, standardize_chunk, 0)

    shrink = 1.0 / samples
    pheno_scaled = standardize_rows(pheno_ref[...])
    scores_ref[...] = dot_nt(scaled[...], pheno_scaled) / jnp.sqrt(jnp.float32(samples))

    def own_block(c, carry):
        rows = pl.ds(c * CHUNK, CHUNK)
        link_ref[rows, total : 2 * total] = (dot_nt(scaled[rows, :], scaled[...]) * shrink).astype(
            jnp.bfloat16
        )
        return carry

    lax.fori_loop(0, chunks, own_block, 0)

    def before(c, carry):
        rows = pl.ds(c * CHUNK, CHUNK)

        @pl.when(has_prev)
        def _():
            forward(c).wait_recv()
            product = (dot_nt(rx[rows, :], scaled[...]) * shrink).astype(jnp.bfloat16)
            ret_out[rows, :] = product
            backward(c).start()

        return carry

    lax.fori_loop(0, chunks, before, 0)

    @pl.when(has_prev)
    def _():
        link_ref[:, :total] = (dot_nt(scaled[...], rx[...]) * shrink).astype(jnp.bfloat16)

    @pl.when(jnp.logical_not(has_prev))
    def _():
        link_ref[:, :total] = jnp.zeros((total, total), jnp.bfloat16)

    @pl.when(jnp.logical_not(has_next))
    def _():
        link_ref[:, 2 * total :] = jnp.zeros((total, total), jnp.bfloat16)

    def drain(s, carry):
        for kind in range(PEER + 3):

            @pl.when(sends[kind])
            def _():
                out_copy(kind, s).wait_send()

        return carry

    lax.fori_loop(0, rounds, drain, 0)

    def after(c, carry):
        rows = pl.ds(c * CHUNK, CHUNK)

        @pl.when(has_next)
        def _():
            backward(c).wait_recv()
            link_ref[rows, 2 * total :] = ret_in[rows, :]
            forward(c).wait_send()

        @pl.when(has_prev)
        def _():
            backward(c).wait_send()

        return carry

    lax.fori_loop(0, chunks, after, 0)


def on_device(n, genotypes, weights, starts, ends, phenotypes):
    samples, cols = genotypes.shape
    genes, tissues, span = weights.shape
    total = genes * tissues
    slots = span // cols + 2
    rounds = samples // ROUND
    chunks = total // CHUNK
    vmem = pl.BlockSpec(memory_space=pltpu.VMEM)
    smem = pl.BlockSpec(memory_space=pltpu.SMEM)
    hbm = pl.BlockSpec(memory_space=pl.ANY)
    dma = pltpu.SemaphoreType.DMA
    traits = phenotypes.shape[1]
    scores, linkage = pl.pallas_call(
        functools.partial(kernel, n),
        out_shape=(
            jax.ShapeDtypeStruct((total, traits), jnp.float32),
            jax.ShapeDtypeStruct((total, 3 * total), jnp.bfloat16),
        ),
        in_specs=[smem, smem, hbm, hbm, vmem],
        out_specs=(vmem, vmem),
        scratch_shapes=[
            pltpu.VMEM((genes, tissues, span), jnp.float32),
            pltpu.VMEM((slots, samples, cols), jnp.bfloat16),
            pltpu.VMEM((total, span + cols), jnp.bfloat16),
            pltpu.VMEM((total, samples), jnp.float32),
            pltpu.VMEM((total, samples), jnp.bfloat16),
            pltpu.VMEM((total, samples), jnp.bfloat16),
            pltpu.VMEM((total, total), jnp.bfloat16),
            pltpu.VMEM((total, total), jnp.bfloat16),
            dma((genes,)),
            dma,
            dma((PEER + 3, rounds)),
            dma((PEER + 3, rounds)),
            dma((chunks,)),
            dma((chunks,)),
            dma((chunks,)),
            dma((chunks,)),
        ],
        compiler_params=pltpu.CompilerParams(
            collective_id=0, has_side_effects=True, vmem_limit_bytes=60 * 1024 * 1024
        ),
    )(starts, ends, genotypes, weights, phenotypes.T)
    return scores.reshape(genes, -1), linkage


def solution(mesh):
    placed = (
        P(None, ("chrom", "var")),
        P(("chrom", "var"), None, None),
        P(("chrom", "var")),
        P(("chrom", "var")),
        P(),
    )
    return jax.shard_map(
        functools.partial(on_device, mesh.shape["var"]),
        mesh=mesh,
        in_specs=placed,
        out_specs=(P(("chrom", "var"), None), P(("chrom", "var"), None)),
        check_vma=False,
    )
```
